32 devices in a mesh: seq: 8 (over z, y), chan: 4 (over x, core).
Axes of the slice: x: 2, y: 2, z: 4, core: 2. Of those that a mesh axis runs over, the one named last changes fastest.
Arguments:
- features: bfloat16 [98304, 1024], P('seq', 'chan'), may hold values from -6 to 6
- gate_input: bfloat16 [98304, 1024], P('seq', 'chan'), may hold values from -6 to 6
- input_map: bfloat16 [98304, 128], P('seq', 'chan'), may hold values from -6 to 6
- output_map: bfloat16 [98304, 128], P('seq', 'chan'), may hold values from -6 to 6
- step_raw: float32 [98304, 16], P('seq', 'chan'), may hold values from -4 to 4
- step_bias: float32 [16], P('chan')
- decay_log: float32 [16], P('chan')
- skip_gain: float32 [16], P('chan'), may hold values from 0.5 to 1.5
- norm_gain: float32 [1024], P('chan'), may hold values from 0.1 to 1.9
- tissue: int32 [192, 2], P('seq'), may hold values from 0 to 512, as said below
Outputs:
- mixed: bfloat16 [98304, 1024], P('seq', 'chan')
The draws below stay inside these ranges and needn't reach their ends.
Inputs may be any that keep to these rules, and one draw needn't show every extreme that they name: tissue[r, 0] <= tissue[r, 1]; a row with equal values holds no tissue.
All inputs are finite; a program needn't handle non-finite values.
Results may differ from the reference program's by a relative error of at most 0.0039.
Values may be sent and summed in bfloat16 or wider, within the bound.
A program may use at most 192 MiB of HBM per device.

```python
import jax
import jax.numpy as jnp
from jax import lax

D = 1024
HEAD = 64
STATE = 128
ROW = 512
HEADS = 16
TOKENS = 98304


def head_kinds(key):
    share = 0.5
    return jax.random.uniform(jax.random.fold_in(key, 11), (HEADS,), jnp.float32) < share


def draw_step_bias(key, part):
    slow = head_kinds(key)
    spread = jax.random.uniform(jax.random.fold_in(key, 21), (HEADS,), jnp.float32)
    return jnp.where(slow, -9.5 + 1.3 * spread, -4.2 + 1.4 * spread).astype(jnp.float32)


def draw_decay_log(key, part):
    slow = head_kinds(key)
    spread = jax.random.uniform(jax.random.fold_in(key, 31), (HEADS,), jnp.float32)
    fast_log = -0.7 + 1.4 * spread
    slow_log = jnp.log((0.5 + spread) / (TOKENS * 0.0001))
    return jnp.where(slow, slow_log, fast_log).astype(jnp.float32)


def draw_tissue(key, part):
    row_count = TOKENS // ROW
    first = jax.random.randint(jax.random.fold_in(key, 41), (row_count,), 0, ROW // 2 + 1)
    last = jax.random.randint(jax.random.fold_in(key, 42), (row_count,), ROW // 2, ROW + 1)
    empty = jax.random.randint(jax.random.fold_in(key, 43), (row_count,), 0, 4) == 0
    last = jnp.where(empty, first, last)
    return jnp.stack([first, last], axis=1).astype(jnp.int32)


def shard_levels(key, dims, cuts, smallest, largest):
    def one(axis_at, shards_of):
        draws = jax.random.uniform(jax.random.fold_in(jax.random.fold_in(key, 6), axis_at), (shards_of,), jnp.float32, smallest / len(cuts), largest / len(cuts))
        return jnp.repeat(jnp.exp(draws), dims[axis_at] // shards_of).reshape((-1,) + (1,) * (len(dims) - axis_at - 1))

    gain = one(*cuts[0])
    for cut in cuts[1:]:
        gain = gain * one(*cut)
    return gain


def scatter_about(rng, extent, scale, most, cuts=(), kind=jnp.bfloat16):
    values = scale * jax.random.normal(rng, extent, jnp.float32)
    if cuts:
        values = values * shard_levels(rng, extent, cuts, -0.22, 0.18)
    return jnp.clip(values, -most, most).astype(kind)


def setup_inputs(seed: int = 0) -> dict:
    splits = jax.random.split(jax.random.key(seed), 11)
    return {
        "features": scatter_about(splits[0], (TOKENS, D), 1.0, 6.0, ((0, 8), (1, 4))),
        "gate_input": scatter_about(splits[1], (TOKENS, D), 1.0, 6.0, ((0, 8), (1, 4))),
        "input_map": scatter_about(splits[2], (TOKENS, STATE), 1.0, 6.0, ((0, 8), (1, 4))),
        "output_map": scatter_about(splits[3], (TOKENS, STATE), 1.0, 6.0, ((0, 8), (1, 4))),
        "step_raw": scatter_about(splits[4], (TOKENS, HEADS), 0.7, 4.0, ((0, 8), (1, 4)), jnp.float32),
        "step_bias": draw_step_bias(jax.random.fold_in(splits[10], 71), 0),
        "decay_log": draw_decay_log(jax.random.fold_in(splits[10], 71), 0),
        "skip_gain": jnp.clip(0.5 + 1.0 * jax.random.uniform(splits[7], (HEADS,), jnp.float32) ** shard_levels(splits[7], (HEADS,), ((0, 4),), -0.2, 0.2), 0.5, 1.5),
        "norm_gain": jnp.clip(1.0 + 0.18 * jax.random.normal(splits[8], (D,), jnp.float32), 0.1, 1.9),
        "tissue": draw_tissue(jax.random.fold_in(splits[10], 71), 0),
    }


EPS = 1e-05

def row_block(state_in, items):
    x_row, gate_row, b_row, c_row, log_row, step_row = items
    running = jnp.cumsum(log_row, axis=0)
    length = log_row.shape[0]
    order = jnp.arange(length, dtype=jnp.int32)
    causal = (order[:, None] >= order[None, :])[None]
    scores = jnp.dot(c_row, b_row.T, preferred_element_type=jnp.float32)
    per_head = running.T
    gap_log = per_head[:, :, None] - per_head[:, None, :]
    damping = jnp.where(causal, jnp.exp(jnp.where(causal, gap_log, 0.0)), 0.0)
    weights = (scores[None] * damping * step_row.T[:, None, :]).astype(jnp.bfloat16)
    x_wide = x_row.astype(jnp.float32)
    inner = jnp.einsum('hts,shp->thp', weights.astype(jnp.float32), x_wide, precision=lax.Precision.HIGHEST)
    carried = jnp.exp(running)[:, :, None] * jnp.einsum('tn,hnp->thp', c_row.astype(jnp.float32), state_in, precision=lax.Precision.HIGHEST)
    row_total = running[-1]
    scaled = jnp.exp(row_total[None, :] - running) * step_row
    b_scaled = (scaled.T[:, :, None] * b_row.astype(jnp.float32)[None]).astype(jnp.bfloat16)
    state_out = jnp.exp(row_total)[:, None, None] * state_in + jnp.einsum('hsn,shp->hnp', b_scaled.astype(jnp.float32), x_wide, precision=lax.Precision.HIGHEST)
    return (state_out, (inner + carried, gate_row))

def reference(features, gate_input, input_map, output_map, step_raw, step_bias, decay_log, skip_gain, norm_gain, tissue):
    row_count = TOKENS // ROW
    position = jnp.arange(ROW, dtype=jnp.int32)
    inside = ((position[None, :] >= tissue[:, 0:1]) & (position[None, :] < tissue[:, 1:2])).astype(jnp.float32)
    step_size = jax.nn.softplus(step_raw.reshape(row_count, ROW, HEADS) + step_bias) * inside[:, :, None]
    log_decay = -jnp.exp(decay_log) * step_size
    x_rows = features.reshape(row_count, ROW, HEADS, HEAD)
    gate_rows = gate_input.reshape(row_count, ROW, D)
    b_rows = input_map.reshape(row_count, ROW, STATE)
    c_rows = output_map.reshape(row_count, ROW, STATE)
    start = jnp.zeros((HEADS, STATE, HEAD), jnp.float32)

    def one_row(state_in, items):
        state_out, (scan_row, gate_row) = row_block(state_in, items)
        y_row = scan_row + skip_gain[:, None] * items[0].astype(jnp.float32)
        gated = y_row.reshape(ROW, D) * jax.nn.silu(gate_row.astype(jnp.float32))
        mean_square = lax.optimization_barrier(jnp.mean(gated * gated, axis=-1, keepdims=True))
        return (state_out, (gated * lax.rsqrt(mean_square + EPS) * norm_gain).astype(jnp.bfloat16))
    _, mixed_rows = lax.scan(one_row, start, (x_rows, gate_rows, b_rows, c_rows, log_decay, step_size))
    return mixed_rows.reshape(TOKENS, D)
```

```python
import functools

import jax
import jax.numpy as jnp
from jax import lax
from jax.experimental import pallas as pl
from jax.experimental.pallas import tpu as pltpu
from jax.sharding import PartitionSpec as P

D = 1024
ROW = 512
EPS = 1e-05
Q = 256
HALF = 128
PAD = 8
LOG2E = 1.4426950408889634
F32 = jnp.float32
BF16 = jnp.bfloat16


def split(v, parts):
    out = []
    for _ in range(parts):
        part = lax.reduce_precision(v, 8, 7)
        out.append(part)
        v = v - part
    return out


def put_heads(xb_ref, x, heads, width):
    lane = lax.broadcasted_iota(jnp.int32, (1, HALF), 1)
    for h in range(heads):
        tile = h * width // HALF
        first = h * width - tile * HALF
        mask = ((lane >= first) & (lane < first + width)).astype(BF16)
        cols = slice(tile * HALF, (tile + 1) * HALF)
        xb_ref[h * Q : (h + 1) * Q, cols] = x[:, cols] * mask


def state_kernel(
    axis, n, heads, width, x_ref, b_ref, rows_ref, dec_ref, tot_ref, out_ref,
    xb, st, slots, send_sem, recv_sem,
):
    step = pl.program_id(0)
    last = pl.num_programs(0) - 1
    me = lax.axis_index(axis)
    states = b_ref.shape[0]

    @pl.when(step == 0)
    def _():
        barrier = pltpu.get_barrier_semaphore()
        for k in range(1, n):
            pl.semaphore_signal(barrier, inc=1, device_id={axis: lax.rem(me + k, n)})
        xb[...] = jnp.zeros_like(xb)
        st[...] = jnp.zeros_like(st)
        st[states : states + PAD, :] = jnp.broadcast_to(tot_ref[...], (PAD, st.shape[1]))

    chunks = x_ref.shape[0] // Q
    state = st[0:states, :]
    for c in range(chunks):
        at = slice(c * Q, (c + 1) * Q)
        put_heads(xb.at[c % 2], x_ref[at, :], heads, width)
        b = b_ref[:, at].astype(F32)
        coef = rows_ref[PAD : 2 * PAD, at]
        bs = jnp.concatenate(
            [(b * coef[h : h + 1, :]).astype(BF16) for h in range(heads)], axis=1
        )
        fresh = jnp.dot(bs, xb[c % 2], preferred_element_type=F32)
        state = state * dec_ref[pl.ds(step * chunks + c, 1), :] + fresh
    st[0:states, :] = state

    @pl.when(step == last)
    def _():
        barrier = pltpu.get_barrier_semaphore()
        pl.semaphore_wait(barrier, n - 1)
        copies = []
        for k in range(1, n):
            copy = pltpu.make_async_remote_copy(
                src_ref=st,
                dst_ref=slots.at[k],
                send_sem=send_sem.at[k],
                recv_sem=recv_sem.at[k],
                device_id={axis: lax.rem(me + k, n)},
            )
            copy.start()
            copies.append(copy)
        for copy in copies:
            copy.wait()
        total = jnp.zeros((states, st.shape[1]), F32)
        for k in range(n - 1, 0, -1):
            live = (k <= me).astype(F32)
            got = slots[k]
            total = total * jnp.exp2(got[states : states + 1, :] * live) + got[0:states, :] * live
        out_ref[...] = total


def band_state(x, b_all, rows, dec, tot, axis, n, heads, width):
    tokens, lanes = x.shape
    states = b_all.shape[0]
    block = 2048 if tokens % 2048 == 0 else ROW
    return pl.pallas_call(
        functools.partial(state_kernel, axis, n, heads, width),
        grid=(tokens // block,),
        in_specs=[
            pl.BlockSpec((block, lanes), lambda i: (i, 0)),
            pl.BlockSpec((states, block), lambda i: (0, i)),
            pl.BlockSpec((2 * PAD, block), lambda i: (0, i)),
            pl.BlockSpec(dec.shape, lambda i: (0, 0)),
            pl.BlockSpec((1, lanes), lambda i: (0, 0)),
        ],
        out_specs=pl.BlockSpec((states, lanes), lambda i: (0, 0)),
        out_shape=jax.ShapeDtypeStruct((states, lanes), F32),
        scratch_shapes=[
            pltpu.VMEM((2, heads * Q, lanes), BF16),
            pltpu.VMEM((states + PAD, lanes), F32),
            pltpu.VMEM((n, states + PAD, lanes), F32),
            pltpu.SemaphoreType.DMA((n,)),
            pltpu.SemaphoreType.DMA((n,)),
        ],
        compiler_params=pltpu.CompilerParams(
            collective_id=1, has_side_effects=True, vmem_limit_bytes=40 * 2**20
        ),
        cost_estimate=pl.CostEstimate(
            flops=2 * tokens * heads * states * lanes,
            bytes_accessed=tokens * (lanes + states) * 2,
            transcendentals=0,
        ),
        name="band_state",
    )(x, b_all, rows, dec, tot)


def scan_kernel(
    heads, width, x_ref, g_ref, b_ref, c_ref, rows_ref, cols_ref, sel_ref, dec_ref, in_ref,
    skip_ref, out_ref, sq_ref, lhs, xb, st,
):
    step = pl.program_id(0)
    states = b_ref.shape[0]
    lanes = x_ref.shape[1]

    @pl.when(step == 0)
    def _():
        xb[...] = jnp.zeros_like(xb)
        lhs[...] = jnp.zeros_like(lhs)
        st[...] = in_ref[...]

    chunks = x_ref.shape[0] // Q
    below = lax.broadcasted_iota(jnp.int32, (HALF, HALF), 0) >= lax.broadcasted_iota(
        jnp.int32, (HALF, HALF), 1
    )
    ones = jnp.ones((PAD, 2 * lanes), BF16)
    state = st[...]
    skip = skip_ref[...]
    for c in range(chunks):
        at = slice(c * Q, (c + 1) * Q)
        slot = c % 2
        x = x_ref[at, :]
        put_heads(xb.at[slot], x, heads, width)
        b = b_ref[:, at]
        ct = c_ref[:, at].T
        scores = jnp.dot(ct, b, preferred_element_type=F32)
        rows = rows_ref[:, at]
        wide = lax.dot_general(
            cols_ref[:, at], sel_ref[...], (((0,), (0,)), ((), ())), preferred_element_type=F32
        )
        left = slot * (Q + states)
        bf = b.astype(F32)
        for h in range(heads):
            base = h * Q
            run = wide[:, h * HALF : (h + 1) * HALF]
            near = rows[h : h + 1, 0:HALF]
            far = rows[h : h + 1, HALF:Q]
            lhs[slot, 0:HALF, base : base + HALF] = jnp.where(
                below, scores[0:HALF, 0:HALF] * jnp.exp2(run[0:HALF] - near), 0.0
            ).astype(BF16)
            lhs[slot, HALF:Q, base : base + HALF] = (
                scores[HALF:Q, 0:HALF] * jnp.exp2(run[HALF:Q] - near)
            ).astype(BF16)
            lhs[slot, HALF:Q, base + HALF : base + Q] = jnp.where(
                below, scores[HALF:Q, HALF:Q] * jnp.exp2(run[HALF:Q] - far), 0.0
            ).astype(BF16)
            lhs[slot, Q : Q + states, base : base + Q] = (
                bf * rows[PAD + h : PAD + h + 1, :]
            ).astype(BF16)
        both = jnp.dot(lhs[slot], xb[slot], preferred_element_type=F32)
        high = state.astype(BF16)
        low = (state - high.astype(F32)).astype(BF16)
        carried = jnp.dot(
            jnp.concatenate([ct, ct], axis=1),
            jnp.concatenate([high, low], axis=0),
            preferred_element_type=F32,
        )
        y = both[0:Q] + wide[:, heads * HALF :] * carried + skip * x.astype(F32)
        g = g_ref[at, :].astype(F32)
        half = 0.5 * g
        gated = y * (half + half * jnp.tanh(half))
        out_ref[at, :] = gated
        square = gated * gated
        sq_high = square.astype(BF16)
        sq_low = (square - sq_high.astype(F32)).astype(BF16)
        sq_ref[:, at] = lax.dot_general(
            ones,
            jnp.concatenate([sq_high, sq_low], axis=1),
            (((1,), (1,)), ((), ())),
            preferred_element_type=F32,
        )
        state = state * dec_ref[pl.ds(step * chunks + c, 1), :] + both[Q : Q + states]
    st[...] = state


def gated_scan(x, g, b_all, c_all, rows, cols, sel, dec, incoming, skip, heads, width):
    tokens, lanes = x.shape
    states = b_all.shape[0]
    block = 1024 if tokens % 1024 == 0 else ROW
    whole = lambda a: pl.BlockSpec(a.shape, lambda i: (0, 0))
    return pl.pallas_call(
        functools.partial(scan_kernel, heads, width),
        grid=(tokens // block,),
        in_specs=[
            pl.BlockSpec((block, lanes), lambda i: (i, 0)),
            pl.BlockSpec((block, lanes), lambda i: (i, 0)),
            pl.BlockSpec((states, block), lambda i: (0, i)),
            pl.BlockSpec((states, block), lambda i: (0, i)),
            pl.BlockSpec((2 * PAD, block), lambda i: (0, i)),
            pl.BlockSpec((cols.shape[0], block), lambda i: (0, i)),
            whole(sel),
            whole(dec),
            whole(incoming),
            whole(skip),
        ],
        out_specs=[
            pl.BlockSpec((block, lanes), lambda i: (i, 0)),
            pl.BlockSpec((PAD, block), lambda i: (0, i)),
        ],
        out_shape=[
            jax.ShapeDtypeStruct((tokens, lanes), F32),
            jax.ShapeDtypeStruct((PAD, tokens), F32),
        ],
        scratch_shapes=[
            pltpu.VMEM((2, Q + states, heads * Q), BF16),
            pltpu.VMEM((2, heads * Q, lanes), BF16),
            pltpu.VMEM((states, lanes), F32),
        ],
        compiler_params=pltpu.CompilerParams(vmem_limit_bytes=40 * 2**20),
        cost_estimate=pl.CostEstimate(
            flops=2 * tokens * heads * (Q + states) * lanes,
            bytes_accessed=tokens * (lanes * 2 + states) * 4,
            transcendentals=tokens * heads * Q,
        ),
        name="gated_scan",
    )(x, g, b_all, c_all, rows, cols, sel, dec, incoming, skip)


def per_device(
    seq_size,
    features,
    gate_input,
    input_map,
    output_map,
    step_raw,
    step_bias,
    decay_log,
    skip_gain,
    norm_gain,
    tissue,
):
    b_all = lax.all_gather(input_map.T, "chan", axis=0, tiled=True)
    c_all = lax.all_gather(output_map.T, "chan", axis=0, tiled=True)
    tokens, lanes = features.shape
    heads = step_bias.shape[0]
    width = lanes // heads
    row_count = tokens // ROW
    chunks = tokens // Q
    position = jnp.arange(ROW, dtype=jnp.int32)
    inside = ((position[None, :] >= tissue[:, 0:1]) & (position[None, :] < tissue[:, 1:2])).astype(F32)
    pad = ((0, PAD - heads), (0, 0))
    raw = step_raw.T + step_bias[:, None]
    step = jnp.pad(jax.nn.softplus(raw) * inside.reshape(1, tokens), pad)
    rate = jnp.pad(-jnp.exp(decay_log) * LOG2E, (0, PAD - heads))
    fall = (step * rate[:, None]).reshape(PAD, chunks, Q)
    upper = jnp.triu(jnp.ones((Q, Q), F32))
    running = jnp.einsum("hcs,st->hct", fall, upper, precision=lax.Precision.HIGHEST)
    total = running[:, :, -1:]
    coef = (jnp.exp2(total - running) * step.reshape(PAD, chunks, Q)).reshape(PAD, tokens)
    running = running.reshape(PAD, tokens)
    rows = jnp.concatenate([running - jnp.log2(step), coef], axis=0)
    cols = jnp.concatenate(
        split(running, 3) + split(jnp.exp2(running), 2) + [jnp.zeros_like(running)], axis=0
    ).astype(BF16)
    to_lane = jnp.repeat(jnp.eye(heads, dtype=F32), width, axis=1)
    to_half = jnp.repeat(jnp.eye(heads, dtype=F32), HALF, axis=1)
    rest = ((0, PAD - heads), (0, 0))
    to_lane, to_half = jnp.pad(to_lane, rest), jnp.pad(to_half, rest)
    sel = jnp.concatenate(
        [
            jnp.concatenate([to_half] * 3 + [jnp.zeros_like(to_half)] * 3, axis=0),
            jnp.concatenate(
                [jnp.zeros_like(to_lane)] * 3 + [to_lane] * 2 + [jnp.zeros_like(to_lane)], axis=0
            ),
        ],
        axis=1,
    ).astype(BF16)
    totals = jnp.repeat(total[:heads, :, 0].T, width, axis=1)
    dec = jnp.exp2(totals)
    band_total = jnp.sum(totals, axis=0, keepdims=True)
    incoming = band_state(
        features, b_all, rows, dec, band_total, "seq", seq_size, heads, width
    )
    skip = jnp.repeat(skip_gain, width)[None, :]
    gated, squares = gated_scan(
        features, gate_input, b_all, c_all, rows, cols, sel, dec, incoming, skip, heads, width
    )
    square_sum = lax.psum(squares[0], "chan")
    scale = lax.rsqrt(square_sum / D + EPS)
    return (gated * scale[:, None] * norm_gain).astype(BF16)


def solution(mesh):
    in_specs = (
        P("seq", "chan"),
        P("seq", "chan"),
        P("seq", "chan"),
        P("seq", "chan"),
        P("seq", "chan"),
        P("chan"),
        P("chan"),
        P("chan"),
        P("chan"),
        P("seq", None),
    )
    return jax.shard_map(
        functools.partial(per_device, mesh.shape["seq"]),
        mesh=mesh,
        in_specs=in_specs,
        out_specs=P("seq", "chan"),
        check_vma=False,
    )
```

```python
import functools

import jax
import jax.numpy as jnp
from jax import lax
from jax.experimental import pallas as pl
from jax.experimental.pallas import tpu as pltpu
from jax.sharding import PartitionSpec as P

D = 1024
ROW = 512
EPS = 1e-05
Q = 256
HALF = 128
PAD = 8
LOG2E = 1.4426950408889634
F32 = jnp.float32
BF16 = jnp.bfloat16


def split(v, parts):
    out = []
    for _ in range(parts):
        part = lax.reduce_precision(v, 8, 7)
        out.append(part)
        v = v - part
    return out


def put_heads(xb_ref, x, heads, width):
    lane = lax.broadcasted_iota(jnp.int32, (1, HALF), 1)
    for h in range(heads):
        tile = h * width // HALF
        first = h * width - tile * HALF
        mask = ((lane >= first) & (lane < first + width)).astype(BF16)
        cols = slice(tile * HALF, (tile + 1) * HALF)
        xb_ref[h * Q : (h + 1) * Q, cols] = x[:, cols] * mask


def state_kernel(
    axis, n, heads, width, x_ref, b_ref, rows_ref, dec_ref, tot_ref, out_ref,
    xb, st, sent, slots, send_sem, recv_sem,
):
    step = pl.program_id(0)
    last = pl.num_programs(0) - 1
    me = lax.axis_index(axis)
    states = b_ref.shape[0]

    @pl.when(step == 0)
    def _():
        barrier = pltpu.get_barrier_semaphore()
        for k in range(1, n):
            pl.semaphore_signal(barrier, inc=1, device_id={axis: lax.rem(me + k, n)})
        xb[...] = jnp.zeros_like(xb)
        st[...] = jnp.zeros_like(st)
        tot = jnp.broadcast_to(tot_ref[...], (2 * PAD, st.shape[1]))
        first = tot.astype(BF16).astype(F32)
        second = (tot - first).astype(BF16).astype(F32)
        third = tot - first - second
        row = lax.broadcasted_iota(jnp.int32, tot.shape, 0)
        parts = jnp.where(row == 0, first, jnp.where(row == 1, second, third))
        sent[states : states + 2 * PAD, :] = parts.astype(BF16)

    chunks = x_ref.shape[0] // Q
    state = st[...]
    for c in range(chunks):
        at = slice(c * Q, (c + 1) * Q)
        put_heads(xb.at[c % 2], x_ref[at, :], heads, width)
        b = b_ref[:, at].astype(F32)
        coef = rows_ref[PAD : 2 * PAD, at]
        bs = jnp.concatenate(
            [(b * coef[h : h + 1, :]).astype(BF16) for h in range(heads)], axis=1
        )
        fresh = jnp.dot(bs, xb[c % 2], preferred_element_type=F32)
        state = state * dec_ref[pl.ds(step * chunks + c, 1), :] + fresh
    st[...] = state

    @pl.when(step == last)
    def _():
        sent[0:states, :] = state.astype(BF16)
        barrier = pltpu.get_barrier_semaphore()
        pl.semaphore_wait(barrier, n - 1)
        copies = []
        for k in range(1, n):
            copy = pltpu.make_async_remote_copy(
                src_ref=sent,
                dst_ref=slots.at[k],
                send_sem=send_sem.at[k],
                recv_sem=recv_sem.at[k],
                device_id={axis: lax.rem(me + k, n)},
            )
            copy.start()
            copies.append(copy)
        for copy in copies:
            copy.wait()
        total = jnp.zeros((states, st.shape[1]), F32)
        for k in range(n - 1, 0, -1):
            live = (k <= me).astype(F32)
            got = slots[k, 0:states, :].astype(F32)
            parts = slots[k, states : states + 2 * PAD, :].astype(F32)
            fall = parts[0:1, :] + parts[1:2, :] + parts[2:3, :]
            total = total * jnp.exp2(fall * live) + got * live
        out_ref[...] = total


def band_state(x, b_all, rows, dec, tot, axis, n, heads, width):
    tokens, lanes = x.shape
    states = b_all.shape[0]
    block = 2048 if tokens % 2048 == 0 else ROW
    return pl.pallas_call(
        functools.partial(state_kernel, axis, n, heads, width),
        grid=(tokens // block,),
        in_specs=[
            pl.BlockSpec((block, lanes), lambda i: (i, 0)),
            pl.BlockSpec((states, block), lambda i: (0, i)),
            pl.BlockSpec((2 * PAD, block), lambda i: (0, i)),
            pl.BlockSpec(dec.shape, lambda i: (0, 0)),
            pl.BlockSpec((1, lanes), lambda i: (0, 0)),
        ],
        out_specs=pl.BlockSpec((states, lanes), lambda i: (0, 0)),
        out_shape=jax.ShapeDtypeStruct((states, lanes), F32),
        scratch_shapes=[
            pltpu.VMEM((2, heads * Q, lanes), BF16),
            pltpu.VMEM((states, lanes), F32),
            pltpu.VMEM((states + 2 * PAD, lanes), BF16),
            pltpu.VMEM((n, states + 2 * PAD, lanes), BF16),
            pltpu.SemaphoreType.DMA((n,)),
            pltpu.SemaphoreType.DMA((n,)),
        ],
        compiler_params=pltpu.CompilerParams(
            collective_id=1, has_side_effects=True, vmem_limit_bytes=60 * 2**20
        ),
        cost_estimate=pl.CostEstimate(
            flops=2 * tokens * heads * states * lanes,
            bytes_accessed=tokens * (lanes + states) * 2,
            transcendentals=0,
        ),
        name="band_state",
    )(x, b_all, rows, dec, tot)


def scan_kernel(
    axis, n, heads, width, x_ref, g_ref, b_ref, c_ref, rows_ref, cols_ref, sel_ref, dec_ref, in_ref,
    skip_ref, out_ref, sq_ref, lhs, xb, st, mine, slots, send_sem, recv_sem,
):
    step = pl.program_id(0)
    states = b_ref.shape[0]
    lanes = x_ref.shape[1]

    me = lax.axis_index(axis)

    @pl.when(step == 0)
    def _():
        barrier = pltpu.get_barrier_semaphore()
        for k in range(1, n):
            pl.semaphore_signal(barrier, inc=1, device_id={axis: lax.rem(me + k, n)})
        xb[...] = jnp.zeros_like(xb)
        lhs[...] = jnp.zeros_like(lhs)
        st[...] = in_ref[...]

    chunks = x_ref.shape[0] // Q
    below = lax.broadcasted_iota(jnp.int32, (HALF, HALF), 0) >= lax.broadcasted_iota(
        jnp.int32, (HALF, HALF), 1
    )
    ones = jnp.ones((PAD, 2 * lanes), BF16)
    state = st[...]
    skip = skip_ref[...]
    for c in range(chunks):
        at = slice(c * Q, (c + 1) * Q)
        slot = c % 2
        x = x_ref[at, :]
        put_heads(xb.at[slot], x, heads, width)
        b = b_ref[:, at]
        ct = c_ref[:, at].T
        scores = jnp.dot(ct, b, preferred_element_type=F32)
        rows = rows_ref[:, at]
        wide = lax.dot_general(
            cols_ref[:, at], sel_ref[...], (((0,), (0,)), ((), ())), preferred_element_type=F32
        )
        left = slot * (Q + states)
        bf = b.astype(F32)
        for h in range(heads):
            base = h * Q
            run = wide[:, h * HALF : (h + 1) * HALF]
            near = rows[h : h + 1, 0:HALF]
            far = rows[h : h + 1, HALF:Q]
            lhs[slot, 0:HALF, base : base + HALF] = jnp.where(
                below, scores[0:HALF, 0:HALF] * jnp.exp2(run[0:HALF] - near), 0.0
            ).astype(BF16)
            lhs[slot, HALF:Q, base : base + HALF] = (
                scores[HALF:Q, 0:HALF] * jnp.exp2(run[HALF:Q] - near)
            ).astype(BF16)
            lhs[slot, HALF:Q, base + HALF : base + Q] = jnp.where(
                below, scores[HALF:Q, HALF:Q] * jnp.exp2(run[HALF:Q] - far), 0.0
            ).astype(BF16)
            lhs[slot, Q : Q + states, base : base + Q] = (
                bf * rows[PAD + h : PAD + h + 1, :]
            ).astype(BF16)
        both = jnp.dot(lhs[slot], xb[slot], preferred_element_type=F32)
        high = state.astype(BF16)
        low = (state - high.astype(F32)).astype(BF16)
        carried = jnp.dot(
            jnp.concatenate([ct, ct], axis=1),
            jnp.concatenate([high, low], axis=0),
            preferred_element_type=F32,
        )
        y = both[0:Q] + wide[:, heads * HALF :] * carried + skip * x.astype(F32)
        g = g_ref[at, :].astype(F32)
        half = 0.5 * g
        gated = y * (half + half * jnp.tanh(half))
        out_ref[at, :] = gated
        square = gated * gated
        sq_high = square.astype(BF16)
        sq_low = (square - sq_high.astype(F32)).astype(BF16)
        sums = lax.dot_general(
            ones,
            jnp.concatenate([sq_high, sq_low], axis=1),
            (((1,), (1,)), ((), ())),
            preferred_element_type=F32,
        )
        mine[pl.ds(step * chunks + c, 1), :] = sums[0:1, :]
        state = state * dec_ref[pl.ds(step * chunks + c, 1), :] + both[Q : Q + states]
    st[...] = state

    @pl.when(step == pl.num_programs(0) - 1)
    def _():
        barrier = pltpu.get_barrier_semaphore()
        pl.semaphore_wait(barrier, n - 1)
        copies = []
        for k in range(1, n):
            copy = pltpu.make_async_remote_copy(
                src_ref=mine,
                dst_ref=slots.at[k],
                send_sem=send_sem.at[k],
                recv_sem=recv_sem.at[k],
                device_id={axis: lax.rem(me + k, n)},
            )
            copy.start()
            copies.append(copy)
        for copy in copies:
            copy.wait()
        total = mine[...]
        for k in range(1, n):
            total = total + slots[k]
        sq_ref[...] = total


def gated_scan(
    x, g, b_all, c_all, rows, cols, sel, dec, incoming, skip, axis, n, heads, width
):
    tokens, lanes = x.shape
    states = b_all.shape[0]
    block = 1024 if tokens % 1024 == 0 else ROW
    whole = lambda a: pl.BlockSpec(a.shape, lambda i: (0, 0))
    return pl.pallas_call(
        functools.partial(scan_kernel, axis, n, heads, width),
        grid=(tokens // block,),
        in_specs=[
            pl.BlockSpec((block, lanes), lambda i: (i, 0)),
            pl.BlockSpec((block, lanes), lambda i: (i, 0)),
            pl.BlockSpec((states, block), lambda i: (0, i)),
            pl.BlockSpec((states, block), lambda i: (0, i)),
            pl.BlockSpec((2 * PAD, block), lambda i: (0, i)),
            pl.BlockSpec((cols.shape[0], block), lambda i: (0, i)),
            whole(sel),
            whole(dec),
            whole(incoming),
            whole(skip),
        ],
        out_specs=[
            pl.BlockSpec((block, lanes), lambda i: (i, 0)),
            pl.BlockSpec((tokens // Q, Q), lambda i: (0, 0)),
        ],
        out_shape=[
            jax.ShapeDtypeStruct((tokens, lanes), F32),
            jax.ShapeDtypeStruct((tokens // Q, Q), F32),
        ],
        scratch_shapes=[
            pltpu.VMEM((2, Q + states, heads * Q), BF16),
            pltpu.VMEM((2, heads * Q, lanes), BF16),
            pltpu.VMEM((states, lanes), F32),
            pltpu.VMEM((tokens // Q, Q), F32),
            pltpu.VMEM((n, tokens // Q, Q), F32),
            pltpu.SemaphoreType.DMA((n,)),
            pltpu.SemaphoreType.DMA((n,)),
        ],
        compiler_params=pltpu.CompilerParams(
            collective_id=2, has_side_effects=True, vmem_limit_bytes=60 * 2**20
        ),
        cost_estimate=pl.CostEstimate(
            flops=2 * tokens * heads * (Q + states) * lanes,
            bytes_accessed=tokens * (lanes * 2 + states) * 4,
            transcendentals=tokens * heads * Q,
        ),
        name="gated_scan",
    )(x, g, b_all, c_all, rows, cols, sel, dec, incoming, skip)


def per_device(
    seq_size,
    chan_size,
    features,
    gate_input,
    input_map,
    output_map,
    step_raw,
    step_bias,
    decay_log,
    skip_gain,
    norm_gain,
    tissue,
):
    b_all = lax.all_gather(input_map.T, "chan", axis=0, tiled=True)
    c_all = lax.all_gather(output_map.T, "chan", axis=0, tiled=True)
    tokens, lanes = features.shape
    heads = step_bias.shape[0]
    width = lanes // heads
    row_count = tokens // ROW
    chunks = tokens // Q
    position = jnp.arange(ROW, dtype=jnp.int32)
    inside = ((position[None, :] >= tissue[:, 0:1]) & (position[None, :] < tissue[:, 1:2])).astype(F32)
    pad = ((0, PAD - heads), (0, 0))
    raw = step_raw.T + step_bias[:, None]
    step = jnp.pad(jax.nn.softplus(raw) * inside.reshape(1, tokens), pad)
    rate = jnp.pad(-jnp.exp(decay_log) * LOG2E, (0, PAD - heads))
    fall = (step * rate[:, None]).reshape(PAD, chunks, Q)
    upper = jnp.triu(jnp.ones((Q, Q), F32))
    running = jnp.einsum("hcs,st->hct", fall, upper, precision=lax.Precision.HIGHEST)
    total = running[:, :, -1:]
    coef = (jnp.exp2(total - running) * step.reshape(PAD, chunks, Q)).reshape(PAD, tokens)
    running = running.reshape(PAD, tokens)
    rows = jnp.concatenate([running - jnp.log2(step), coef], axis=0)
    cols = jnp.concatenate(
        split(running, 3) + split(jnp.exp2(running), 2) + [jnp.zeros_like(running)], axis=0
    ).astype(BF16)
    to_lane = jnp.repeat(jnp.eye(heads, dtype=F32), width, axis=1)
    to_half = jnp.repeat(jnp.eye(heads, dtype=F32), HALF, axis=1)
    rest = ((0, PAD - heads), (0, 0))
    to_lane, to_half = jnp.pad(to_lane, rest), jnp.pad(to_half, rest)
    sel = jnp.concatenate(
        [
            jnp.concatenate([to_half] * 3 + [jnp.zeros_like(to_half)] * 3, axis=0),
            jnp.concatenate(
                [jnp.zeros_like(to_lane)] * 3 + [to_lane] * 2 + [jnp.zeros_like(to_lane)], axis=0
            ),
        ],
        axis=1,
    ).astype(BF16)
    totals = jnp.repeat(total[:heads, :, 0].T, width, axis=1)
    dec = jnp.exp2(totals)
    band_total = jnp.sum(totals, axis=0, keepdims=True)
    incoming = band_state(
        features, b_all, rows, dec, band_total, "seq", seq_size, heads, width
    )
    skip = jnp.repeat(skip_gain, width)[None, :]
    gated, squares = gated_scan(
        features, gate_input, b_all, c_all, rows, cols, sel, dec, incoming, skip,
        "chan", chan_size, heads, width,
    )
    scale = lax.rsqrt(squares.reshape(tokens) / D + EPS)
    return (gated * scale[:, None] * norm_gain).astype(BF16)


def solution(mesh):
    in_specs = (
        P("seq", "chan"),
        P("seq", "chan"),
        P("seq", "chan"),
        P("seq", "chan"),
        P("seq", "chan"),
        P("chan"),
        P("chan"),
        P("chan"),
        P("chan"),
        P("seq", None),
    )
    return jax.shard_map(
        functools.partial(per_device, mesh.shape["seq"], mesh.shape["chan"]),
        mesh=mesh,
        in_specs=in_specs,
        out_specs=P("seq", "chan"),
        check_vma=False,
    )
```
